32 devices in a mesh: replica: 1 (over z), tp: 4 (over y), stage: 8 (over x, core).
Axes of the slice: x: 4, y: 4, z: 1, core: 2. Of those that a mesh axis runs over, the one named last changes fastest.
The devices are a block of a 4x4x8 slice.
Arguments:
- embeds: bfloat16 [32, 2, 2048], P('replica')
- w_qkv: bfloat16 [8, 2048, 8, 4, 128], P('stage', None, 'tp')
- w_out: bfloat16 [8, 2048, 2048], P('stage', 'tp')
- w_gate: bfloat16 [8, 2048, 6144], P('stage', None, 'tp')
- w_up: bfloat16 [8, 2048, 6144], P('stage', None, 'tp')
- w_down: bfloat16 [8, 6144, 2048], P('stage', 'tp')
- norm_gain: float32 [8, 2, 2048], P('stage')
- k_cache: bfloat16 [8, 32, 2, 16, 8, 128], P('stage', 'replica', None, None, 'tp')
- v_cache: bfloat16 [8, 32, 2, 16, 8, 128], P('stage', 'replica', None, None, 'tp')
- lengths: int32 [32, 2], P('replica')
- final_gain: float32 [2048], replicated
- w_unembed: bfloat16 [2048, 151936], P(None, ('stage', 'tp'))
Outputs:
- output 1: float32 [32, 2, 151936], P('replica', None, ('stage', 'tp'))
- output 2: bfloat16 [8, 32, 2, 16, 8, 128], P('stage', 'replica', None, None, 'tp')
- output 3: bfloat16 [8, 32, 2, 16, 8, 128], P('stage', 'replica', None, None, 'tp')
All inputs are finite; a program needn't handle non-finite values.
Results may differ from the reference program's by a relative error of at most 0.02.
Values are sent between devices in bfloat16 or wider.
A program may use at most 768 MiB of HBM per device.

```python
import jax
import jax.numpy as jnp
from jax import lax

D = 2048
HEADS = 16
KV_HEADS = 8
HEAD = 128
FF = 6144
VOCAB = 151936
STAGES = 8
LAYERS_STAGE = 1
GROUPS = 32
BATCH = 2
CTX = 16

LAYERS = LAYERS_STAGE * STAGES
QGROUP = HEADS // KV_HEADS
SLOTS = QGROUP + 2
ROPE_THETA = 10000.0
NORM_EPS = 1e-5


def draw_lengths(len_key):
    low_len = CTX // 4
    tok_count = GROUPS * BATCH
    len_flat = jax.random.randint(len_key, (tok_count,), low_len, CTX, dtype=jnp.int32)
    pick_idx = jax.random.permutation(jax.random.fold_in(len_key, 1), tok_count)
    len_flat = len_flat.at[pick_idx[0]].set(CTX - 1).at[pick_idx[1]].set(low_len)
    return len_flat.reshape(GROUPS, BATCH)


def setup_inputs(seed: int = 0, part: int = 0) -> dict:
    root_key = jax.random.key(seed)
    shared_keys = jax.random.split(root_key, 8)
    part_keys = jax.random.split(jax.random.fold_in(root_key, part), 4)
    embeds = jax.random.normal(part_keys[0], (GROUPS, BATCH, D), jnp.float32).astype(jnp.bfloat16)
    w_qkv = (jax.random.normal(shared_keys[0], (LAYERS, D, KV_HEADS, SLOTS, HEAD), jnp.float32) * D ** -0.5).astype(jnp.bfloat16)
    w_out = (jax.random.normal(shared_keys[1], (LAYERS, HEADS * HEAD, D), jnp.float32) * (HEADS * HEAD) ** -0.5).astype(jnp.bfloat16)
    w_gate = (jax.random.normal(shared_keys[2], (LAYERS, D, FF), jnp.float32) * D ** -0.5).astype(jnp.bfloat16)
    w_up = (jax.random.normal(shared_keys[3], (LAYERS, D, FF), jnp.float32) * D ** -0.5).astype(jnp.bfloat16)
    w_down = (jax.random.normal(shared_keys[4], (LAYERS, FF, D), jnp.float32) * FF ** -0.5).astype(jnp.bfloat16)
    norm_gain = 1.0 + 0.25 * jax.random.normal(shared_keys[5], (LAYERS, 2, D), jnp.float32)
    k_cache = jax.random.normal(part_keys[1], (LAYERS, GROUPS, BATCH, CTX, KV_HEADS, HEAD), jnp.float32).astype(jnp.bfloat16)
    v_cache = jax.random.normal(part_keys[2], (LAYERS, GROUPS, BATCH, CTX, KV_HEADS, HEAD), jnp.float32).astype(jnp.bfloat16)
    lengths = draw_lengths(part_keys[3])
    final_gain = 1.0 + 0.25 * jax.random.normal(shared_keys[6], (D,), jnp.float32)
    w_unembed = (jax.random.normal(shared_keys[7], (D, VOCAB), jnp.float32) * D ** -0.5).astype(jnp.bfloat16)
    return dict(embeds=embeds, w_qkv=w_qkv, w_out=w_out, w_gate=w_gate, w_up=w_up, w_down=w_down, norm_gain=norm_gain, k_cache=k_cache, v_cache=v_cache, lengths=lengths, final_gain=final_gain, w_unembed=w_unembed)


def rms_norm(values, gain_row):
    mean_sq = jnp.mean(values * values, axis=-1, keepdims=True)
    return (values * lax.rsqrt(mean_sq + NORM_EPS) * gain_row).astype(jnp.bfloat16)


def rotate_half(values, cos_part, sin_part):
    half_dim = values.shape[-1] // 2
    first_half = values[..., :half_dim]
    second_half = values[..., half_dim:]
    return jnp.concatenate([first_half * cos_part - second_half * sin_part, second_half * cos_part + first_half * sin_part], axis=-1)


def reference(embeds, w_qkv, w_out, w_gate, w_up, w_down, norm_gain, k_cache, v_cache, lengths, final_gain, w_unembed):
    tok_count = GROUPS * BATCH
    inv_freq = ROPE_THETA ** (-jnp.arange(HEAD // 2, dtype=jnp.float32) * (2.0 / HEAD))
    angles = lengths.astype(jnp.float32)[..., None] * inv_freq
    cos_part = jnp.cos(angles)
    sin_part = jnp.sin(angles)
    cos_q = cos_part[:, :, None, None, :]
    sin_q = sin_part[:, :, None, None, :]
    cos_k = cos_part[:, :, None, :]
    sin_k = sin_part[:, :, None, :]
    positions = jnp.arange(CTX)
    write_hit = (positions[None, None, :] == lengths[:, :, None])[:, :, :, None, None]
    visible = (positions[None, None, :] <= lengths[:, :, None])[:, :, None, None, :]
    stage_end = (jnp.arange(LAYERS) % LAYERS_STAGE) == LAYERS_STAGE - 1

    def layer_step(residual, layer_in):
        wq_layer, wo_layer, wg_layer, wu_layer, wd_layer, gain_pair, k_layer, v_layer, at_end = layer_in
        normed = rms_norm(residual, gain_pair[0]).reshape(tok_count, D)
        proj_out = jnp.dot(normed, wq_layer.reshape(D, KV_HEADS * SLOTS * HEAD), preferred_element_type=jnp.float32)
        proj_out = proj_out.reshape(GROUPS, BATCH, KV_HEADS, SLOTS, HEAD)
        queries = rotate_half(proj_out[:, :, :, :QGROUP], cos_q, sin_q).astype(jnp.bfloat16)
        key_new = rotate_half(proj_out[:, :, :, QGROUP], cos_k, sin_k).astype(jnp.bfloat16)
        val_new = proj_out[:, :, :, QGROUP + 1].astype(jnp.bfloat16)
        k_upd = jnp.where(write_hit, key_new[:, :, None], k_layer)
        v_upd = jnp.where(write_hit, val_new[:, :, None], v_layer)
        scores = jnp.einsum('gbkqn,gbtkn->gbkqt', queries.astype(jnp.float32), k_upd.astype(jnp.float32)) * HEAD ** -0.5
        scores = jnp.where(visible, scores, -jnp.inf)
        attn_probs = jax.nn.softmax(scores, axis=-1).astype(jnp.bfloat16)
        attn_out = jnp.einsum('gbkqt,gbtkn->gbkqn', attn_probs.astype(jnp.float32), v_upd.astype(jnp.float32)).astype(jnp.bfloat16)
        residual = residual + jnp.dot(attn_out.reshape(tok_count, HEADS * HEAD), wo_layer, preferred_element_type=jnp.float32).reshape(GROUPS, BATCH, D)
        normed_mlp = rms_norm(residual, gain_pair[1]).reshape(tok_count, D)
        gate_act = jnp.dot(normed_mlp, wg_layer, preferred_element_type=jnp.float32)
        up_act = jnp.dot(normed_mlp, wu_layer, preferred_element_type=jnp.float32)
        hidden = (jax.nn.silu(gate_act) * up_act).astype(jnp.bfloat16)
        residual = residual + jnp.dot(hidden, wd_layer, preferred_element_type=jnp.float32).reshape(GROUPS, BATCH, D)
        residual = jnp.where(at_end, residual.astype(jnp.bfloat16).astype(jnp.float32), residual)
        return residual, (k_upd, v_upd)

    final_res, cache_pair = lax.scan(layer_step, embeds.astype(jnp.float32), (w_qkv, w_out, w_gate, w_up, w_down, norm_gain, k_cache, v_cache, stage_end))
    normed_out = rms_norm(final_res, final_gain).reshape(tok_count, D)
    logits = jnp.dot(normed_out, w_unembed, preferred_element_type=jnp.float32).reshape(GROUPS, BATCH, VOCAB)
    return logits, cache_pair[0], cache_pair[1]
```

```python
import functools

import numpy as np
import jax
import jax.numpy as jnp
from jax import lax
from jax.experimental import pallas as pl
from jax.experimental.pallas import tpu as pltpu
from jax.sharding import PartitionSpec as P

NORM_EPS = 1e-5
ROPE_THETA = 10000.0
ROWS = 8
F32 = jnp.float32
BF16 = jnp.bfloat16
MESH = pl.DeviceIdType.MESH


def rope_rows(positions, head_dim):
    half = head_dim // 2
    inv_freq = (np.float32(ROPE_THETA) ** (-np.arange(half, dtype=np.float32) * np.float32(2.0 / head_dim))).astype(np.float32)
    angles = np.arange(positions, dtype=np.float32)[:, None] * inv_freq[None, :]
    cos, sin = np.cos(angles), np.sin(angles)
    return np.stack([np.concatenate([cos, cos], -1), np.concatenate([-sin, sin], -1)]).astype(np.float32)


def normed(values, gain):
    mean_sq = jnp.mean(values * values, axis=-1, keepdims=True)
    return (values * lax.rsqrt(mean_sq + NORM_EPS) * gain).astype(BF16)


def step_kernel(dims, emb, wq_raw, wo_h, wg_h, wu_h, wd_h, gains_h, kc_h, vc_h, lens, rope_h, fgain_h, wv_h,
                logits_h, ko_h, vo_h,
                raw, stage32, wq, wo, wg, wu, wd, gains, kc, vc, rope, fgain, wv, rin, res, hid, ar1, part, rs2, outs, fin, cosb, sinb, xn, logits,
                ld, ldq, lo, ar1_s, ar1_r, rs2_s, rs2_r, ag_s, ag_r, fin_s, fin_r):
    tp, stages, chunks, kvs, slots, hd, ctx = dims
    qpk = slots - 2
    nh = kvs * qpk
    width = wo.shape[1]
    cw = width // tp
    ff = wg.shape[1]
    me = lax.axis_index("tp")
    st = lax.axis_index("stage")
    total = tp * stages
    mine = st * tp + me
    last = stages - 1
    krows = ROWS * ctx * kvs

    def dev(flat):
        return {"stage": flat // tp, "tp": lax.rem(flat, tp)}

    cpl = lambda s, d, k: pltpu.make_async_copy(s, d, ld.at[k])
    qrows = raw.shape[0] // 8
    qc = [pltpu.make_async_copy(wq_raw.at[pl.ds(i * qrows, qrows)], raw.at[pl.ds(i * qrows, qrows)], ldq.at[i]) for i in range(8)]
    loads = [cpl(gains_h, gains, 0), cpl(rope_h, rope, 1), cpl(kc_h, kc, 2), cpl(vc_h, vc, 3), cpl(wo_h, wo, 4), cpl(wg_h, wg, 5), cpl(wu_h, wu, 6), cpl(wd_h, wd, 7), cpl(fgain_h, fgain, 8), cpl(wv_h, wv, 9)]
    emb_load = cpl(emb, rin, 10)

    for c in qc[:2]:
        c.start()

    @pl.when(st == 0)
    def _():
        emb_load.start()

    for c in loads[:2]:
        c.start()
    for c in qc[2:]:
        c.start()
    for c in loads[2:]:
        c.start()

    barrier = pltpu.get_barrier_semaphore()

    def greet(k, _):
        pl.semaphore_signal(barrier, inc=1, device_id=dev(lax.rem(mine + k, total)), device_id_type=MESH)
        return 0

    lax.fori_loop(1, total, greet, 0)

    row8 = lax.broadcasted_iota(jnp.int32, (ROWS, hd), 0)

    def lens_of(c):
        return [lens[i % 2, c * (ROWS // 2) + i // 2] for i in range(ROWS)]

    loads[1].wait()

    def rope_body(c, _):
        len8 = jnp.zeros((ROWS, hd), jnp.int32)
        for i, v in enumerate(lens_of(c)):
            len8 = jnp.where(row8 == i, v, len8)
        cs = jnp.zeros((ROWS, hd), F32)
        sn = jnp.zeros((ROWS, hd), F32)
        for p in range(ctx):
            cs = jnp.where(len8 == p, rope[0, p:p + 1, :], cs)
            sn = jnp.where(len8 == p, rope[1, p:p + 1, :], sn)
        cosb[c] = cs
        sinb[c] = sn
        return 0

    lax.fori_loop(0, chunks, rope_body, 0)

    nslot = kvs * slots
    kq = qrows // nslot
    for i in range(8):
        qc[i].wait()
        stage32[...] = raw[pl.ds(i * qrows, qrows), :].astype(F32)
        for s in range(nslot):
            wq[pl.ds(i * kq, kq), pl.ds(s * hd, hd)] = stage32[pl.ds(s, kq, stride=nslot), :].astype(BF16)

    loads[0].wait()

    @pl.when(st == 0)
    def _():
        emb_load.wait()

    pl.semaphore_wait(barrier, total - 1)

    scale = hd ** -0.5

    def ar1_copy(c, slot, d, peer):
        return pltpu.make_async_remote_copy(src_ref=ar1.at[c, slot], dst_ref=ar1.at[c, slot], send_sem=ar1_s.at[c, d], recv_sem=ar1_r.at[c, slot], device_id={"tp": peer}, device_id_type=MESH)

    def rs2_copy(c, slot, d, peer):
        return pltpu.make_async_remote_copy(src_ref=part.at[c, peer], dst_ref=rs2.at[c, slot], send_sem=rs2_s.at[c, d], recv_sem=rs2_r.at[c, slot], device_id={"tp": peer}, device_id_type=MESH)

    def ag_copy(c, slot, d, peer, nxt):
        return pltpu.make_async_remote_copy(src_ref=outs.at[c], dst_ref=rin.at[c, slot], send_sem=ag_s.at[c, d], recv_sem=ag_r.at[c, slot], device_id={"stage": nxt, "tp": peer}, device_id_type=MESH)

    def fin_copy(c, slot, flat):
        return pltpu.make_async_remote_copy(src_ref=outs.at[c], dst_ref=fin.at[c * tp + slot], send_sem=fin_s.at[c], recv_sem=fin_r.at[c, slot], device_id=dev(flat), device_id_type=MESH)

    def attn_part(c):
        @pl.when(st > 0)
        def _():
            for s in range(tp):
                ag_copy(c, s, s, s, 0).wait_recv()

        x = jnp.concatenate([rin[c, s] for s in range(tp)], axis=1).astype(F32)
        u = normed(x, gains[0:1, :])
        proj = jnp.dot(u, wq[...], preferred_element_type=F32)
        cs, sn = cosb[c], sinb[c]

        def rot(v):
            return v * cs + pltpu.roll(v, hd // 2, 1) * sn

        qs, kn, vn = [], [], []
        for kv in range(kvs):
            for j in range(slots):
                o = (kv * slots + j) * hd
                v = proj[:, o:o + hd]
                if j < qpk:
                    qs.append(rot(v))
                elif j == qpk:
                    kn.append(rot(v).astype(BF16).astype(F32))
                else:
                    vn.append(v.astype(BF16).astype(F32))
        qb = jnp.concatenate(qs, axis=0).astype(BF16)
        k_rep = jnp.concatenate([kn[h // qpk] for h in range(nh)], axis=0)
        v_rep = jnp.concatenate([vn[h // qpk] for h in range(nh)], axis=0)

        @pl.when(c == 0)
        def _():
            loads[2].wait()
            loads[3].wait()

        ks = pl.ds(pl.multiple_of(c * krows, krows), krows)
        s_old = lax.dot_general(qb, kc[ks, :], (((1,), (1,)), ((), ())), preferred_element_type=F32) * scale
        s_new = jnp.sum(qb.astype(F32) * k_rep, axis=-1, keepdims=True) * scale
        lvals = lens_of(c)
        rr = lax.broadcasted_iota(jnp.int32, (nh * ROWS, krows), 0)
        cc = lax.broadcasted_iota(jnp.int32, (nh * ROWS, krows), 1)
        rs = lax.rem(rr, ROWS)
        lrow = jnp.zeros((nh * ROWS, krows), jnp.int32)
        for i, v in enumerate(lvals):
            lrow = jnp.where(rs == i, v, lrow)
        visible = (rs == cc // (ctx * kvs)) & (rr // (qpk * ROWS) == lax.rem(cc, kvs)) & (lax.rem(cc // kvs, ctx) < lrow)
        s_old = jnp.where(visible, s_old, -1e30)
        peak = jnp.maximum(jnp.max(s_old, axis=-1, keepdims=True), s_new)
        p_old = jnp.where(visible, jnp.exp(s_old - peak), 0.0)
        p_new = jnp.exp(s_new - peak)
        den = jnp.sum(p_old, axis=-1, keepdims=True) + p_new
        pb = (p_old / den).astype(BF16)
        pn = (p_new / den).astype(BF16).astype(F32)
        at = jnp.dot(pb, vc[ks, :], preferred_element_type=F32) + pn * v_rep
        flat = jnp.concatenate([at[h * ROWS:(h + 1) * ROWS, :] for h in range(nh)], axis=1).astype(BF16)

        @pl.when(c == 0)
        def _():
            loads[4].wait()

        ar1[c, me] = jnp.dot(flat, wo[...], preferred_element_type=F32)
        for d in (2, 1, 3):
            ar1_copy(c, me, d, lax.rem(me + d, tp)).start()

        half = lax.broadcasted_iota(jnp.int32, (ctx * kvs, hd), 0)
        sel = lax.rem(half, kvs)
        pos = half // kvs
        for buf, new, out_h, sem in ((kc, kn, ko_h, 0), (vc, vn, vo_h, 1)):
            for i in range(ROWS):
                rows = pl.ds(pl.multiple_of(c * krows + i * ctx * kvs, ctx * kvs), ctx * kvs)
                cand = jnp.broadcast_to(new[0][i:i + 1, :], (ctx * kvs, hd))
                for h in range(1, kvs):
                    cand = jnp.where(sel == h, new[h][i:i + 1, :], cand)
                buf[rows, :] = jnp.where(pos == lvals[i], cand, buf[rows, :].astype(F32)).astype(BF16)
            pltpu.make_async_copy(buf.at[ks], out_h.at[ks], lo.at[sem, c]).start()

    def mlp_up(c):
        for d in range(1, tp):
            s = lax.rem(me + d, tp)
            ar1_copy(c, s, d, s).wait_recv()
        x = jnp.concatenate([rin[c, s] for s in range(tp)], axis=1).astype(F32)
        tot = ar1[c, 0]
        for s in range(1, tp):
            tot = tot + ar1[c, s]
        r = x + tot
        for s in range(tp):
            res[c, s] = r[:, s * cw:(s + 1) * cw]
        u = normed(r, gains[1:2, :])

        @pl.when(c == 0)
        def _():
            loads[5].wait()
            loads[6].wait()

        g = jnp.dot(u, wg[...], preferred_element_type=F32)
        up = jnp.dot(u, wu[...], preferred_element_type=F32)
        hid[...] = (g * jax.nn.sigmoid(g)) * up

    def mlp_down(c):
        @pl.when(c == 0)
        def _():
            loads[7].wait()

        y = jnp.dot(hid[...].astype(BF16), wd[...], preferred_element_type=F32)
        for s in range(tp):
            part[c, s] = y[:, s * cw:(s + 1) * cw]
        for d in (2, 1, 3):
            rs2_copy(c, me, d, lax.rem(me + d, tp)).start()
        rs2[c, me] = part[c, me]

    def stage_end(c):
        for d in range(1, tp):
            s = lax.rem(me + d, tp)
            rs2_copy(c, s, d, s).wait_recv()
        tot = rs2[c, 0]
        for s in range(1, tp):
            tot = tot + rs2[c, s]
        outs[c] = (res[c, me] + tot).astype(BF16)

        @pl.when(st < last)
        def _():
            for d in (2, 1, 3, 0):
                ag_copy(c, me, d, lax.rem(me + d, tp), st + 1).start()

        @pl.when(st == last)
        def _():
            def send(k, _):
                fin_copy(c, me, lax.rem(mine + k, total)).start()
                return 0

            lax.fori_loop(1, total, send, 0)
            fin[c * tp + me] = outs[c]

    def tick(i, _):
        @pl.when(i < chunks)
        def _():
            attn_part(i)

        @pl.when((i >= 1) & (i <= chunks))
        def _():
            mlp_up(i - 1)

        @pl.when(i >= 2)
        def _():
            stage_end(i - 2)

        @pl.when((i >= 1) & (i <= chunks))
        def _():
            mlp_down(i - 1)

        return 0

    lax.fori_loop(0, chunks + 2, tick, 0)

    loads[8].wait()
    for c in range(chunks):
        for s in range(tp):
            @pl.when((st < last) | (me != s))
            def _():
                fin_copy(c, s, s).wait_recv()
    for p in range(chunks // 2):
        rows = [jnp.concatenate([fin[c * tp + s] for s in range(tp)], axis=1).astype(F32) for c in (2 * p, 2 * p + 1)]
        xn[2 * p * ROWS:(2 * p + 2) * ROWS, :] = normed(jnp.concatenate(rows, axis=0), fgain[...])
    loads[9].wait()
    vocab = wv.shape[0]
    tile = 768
    full = vocab // tile

    def vocab_tile(j, _):
        o = pl.multiple_of(j * tile, tile)
        logits[:, pl.ds(o, tile)] = lax.dot_general(xn[...], wv[pl.ds(o, tile), :], (((1,), (1,)), ((), ())), preferred_element_type=F32)
        return 0

    lax.fori_loop(0, full, vocab_tile, 0)
    if full * tile < vocab:
        logits[:, full * tile:] = lax.dot_general(xn[...], wv[full * tile:, :], (((1,), (1,)), ((), ())), preferred_element_type=F32)
    out = pltpu.make_async_copy(logits, logits_h, ld.at[11])
    out.start()

    def drain(c, _):
        for d in range(1, tp):
            ar1_copy(c, me, d, lax.rem(me + d, tp)).wait_send()
            rs2_copy(c, me, d, lax.rem(me + d, tp)).wait_send()

        @pl.when(st < last)
        def _():
            for d in range(tp):
                ag_copy(c, me, d, lax.rem(me + d, tp), st + 1).wait_send()

        @pl.when(st == last)
        def _():
            view = fin.at[pl.ds(0, total - 1)]
            pltpu.make_async_copy(view, view, fin_s.at[c]).wait()

        ks = pl.ds(pl.multiple_of(c * krows, krows), krows)
        pltpu.make_async_copy(kc.at[ks], ko_h.at[ks], lo.at[0, c]).wait()
        pltpu.make_async_copy(vc.at[ks], vo_h.at[ks], lo.at[1, c]).wait()
        return 0

    lax.fori_loop(0, chunks, drain, 0)
    out.wait()


def solution(mesh):
    tp, stages = mesh.shape["tp"], mesh.shape["stage"]
    cache_spec = P('stage', 'replica', None, None, 'tp', None)
    in_specs = (P('replica'), P('stage', None, 'tp', None, None), P('stage', 'tp', None), P('stage', None, 'tp'), P('stage', None, 'tp'), P('stage', 'tp', None), P('stage'), cache_spec, cache_spec, P('replica'), P(), P(None, ('stage', 'tp')))
    out_specs = (P('replica', None, ('stage', 'tp')), cache_spec, cache_spec)

    def device_step(embeds, w_qkv, w_out, w_gate, w_up, w_down, norm_gain, k_cache, v_cache, lengths, final_gain, w_unembed):
        groups, batch, width = embeds.shape
        tokens = groups * batch
        chunks = tokens // ROWS
        cw = width // tp
        _, _, kvs, slots, hd = w_qkv.shape
        ctx = k_cache.shape[3]
        ff = w_gate.shape[2]
        vocab = w_unembed.shape[1]
        crow = tokens * ctx * kvs
        emb = embeds.reshape(chunks, ROWS, tp, cw).transpose(0, 2, 1, 3)
        args = (emb, w_qkv.reshape(width * kvs * slots, hd), w_out[0], w_gate[0], w_up[0], w_down[0], norm_gain[0],
                k_cache.reshape(crow, hd), v_cache.reshape(crow, hd), lengths.T, jnp.asarray(rope_rows(ctx, hd)), final_gain.reshape(1, width), w_unembed.T)
        hbm = pl.BlockSpec(memory_space=pl.ANY)
        in_s = [hbm] * len(args)
        in_s[9] = pl.BlockSpec(memory_space=pltpu.SMEM)
        V = pltpu.VMEM
        dma = pltpu.SemaphoreType.DMA
        qtot = width * kvs * slots
        scratch = [V((qtot, hd), BF16), V((qtot // 8, hd), F32), V((width, kvs * slots * hd), BF16), V(w_out.shape[1:], BF16), V(w_gate.shape[1:], BF16), V(w_up.shape[1:], BF16), V(w_down.shape[1:], BF16),
                   V((2, width), F32), V((crow, hd), BF16), V((crow, hd), BF16), V((2, ctx, hd), F32), V((1, width), F32), V((vocab, width), BF16),
                   V((chunks, tp, ROWS, cw), BF16), V((chunks, tp, ROWS, cw), F32), V((ROWS, ff), F32), V((chunks, tp, ROWS, width), F32), V((chunks, tp, ROWS, cw), F32), V((chunks, tp, ROWS, cw), F32),
                   V((chunks, ROWS, cw), BF16), V((chunks * tp, ROWS, cw), BF16), V((chunks, ROWS, hd), F32), V((chunks, ROWS, hd), F32), V((tokens, width), BF16), V((tokens, vocab), F32),
                   dma((12,)), dma((8,)), dma((2, chunks)), dma((chunks, tp)), dma((chunks, tp)), dma((chunks, tp)), dma((chunks, tp)), dma((chunks, tp)), dma((chunks, tp)), dma((chunks,)), dma((chunks, tp))]
        logits, k_out, v_out = pl.pallas_call(
            functools.partial(step_kernel, (tp, stages, chunks, kvs, slots, hd, ctx)),
            out_shape=[jax.ShapeDtypeStruct((tokens, vocab), F32), jax.ShapeDtypeStruct((crow, hd), BF16), jax.ShapeDtypeStruct((crow, hd), BF16)],
            in_specs=in_s, out_specs=[hbm] * 3, scratch_shapes=scratch, name="decode_step",
            compiler_params=pltpu.CompilerParams(collective_id=0, has_side_effects=True, vmem_limit_bytes=67043328))(*args)
        return logits.reshape(groups, batch, vocab), k_out.reshape(k_cache.shape), v_out.reshape(v_cache.shape)

    return jax.shard_map(device_step, mesh=mesh, in_specs=in_specs, out_specs=out_specs, check_vma=False)
```
